32 devices in a mesh: rows: 16 (over z, y, x), cols: 2 (over core).
Axes of the slice: x: 2, y: 2, z: 4, core: 2. Of those that a mesh axis runs over, the one named last changes fastest.
Arguments:
- rhs: float32 [2, 96, 6144], P('cols', 'rows'), may hold values from -6 to 6
- pattern: int32 [48, 2], P(None, 'cols'), may hold values 0 or 1
- front_blocks: int32 [16, 4], replicated, may hold values from 0 to 47, as said below
- front_slot: int32 [16], replicated, may hold values from 0 to 31, as said below
- pivot_inverse: float32 [32, 256, 256], P('rows'), may hold values from -0.375 to 0.375
- update_factor: float32 [32, 256, 256], P('rows'), may hold values from -0.375 to 0.375
Outputs:
- solution: float32 [2, 96, 6144], P('cols', 'rows')
The draws below stay inside these ranges and needn't reach their ends.
Inputs may be any that keep to these rules, and one draw needn't show every extreme that they name: `front_blocks`: columns 0 and 1 together name every row block that is no contribution block exactly once; columns 2 and 3 of a front are two different blocks, never a pivot block of any front. `front_slot`: all different; slot s belongs to index s // 2 of rows; some index holds 2 fronts in every draw; slots that no front names are unused.
All inputs are finite; a program needn't handle non-finite values. No bound on the sum of `pattern` on one device may be relied on, other than what follows from the above.
Results may differ from the reference program's by a relative error of at most 0.0001.
Values sent between devices are 32-bit elements; how exact they have to be, the bound alone decides.
A program may use at most 64 MiB of HBM per device.

```python
import jax
import jax.numpy as jnp
from jax import lax

BLOCK = 128
PIV = 256
SLOT_DEV = 2
FRONTS = 16
SLOTS = 32
RB = 48
NROWS = 6144
GROUPS = 2
GCOLS = 96


def draw_front_blocks(key, part):
    shuffled = jax.random.permutation(jax.random.fold_in(key, 11), RB).astype(jnp.int32)
    pivots = shuffled[:2 * FRONTS].reshape(FRONTS, 2)
    separators = shuffled[2 * FRONTS:]
    first_sep = jax.random.randint(jax.random.fold_in(key, 12), (FRONTS,), 0, FRONTS).astype(jnp.int32)
    stride_draw = jax.random.randint(jax.random.fold_in(key, 13), (FRONTS,), 1, FRONTS).astype(jnp.int32)
    second_sep = (first_sep + stride_draw) % FRONTS
    return jnp.concatenate([pivots, separators[first_sep][:, None], separators[second_sep][:, None]], axis=1).astype(jnp.int32)


def draw_front_slot(key, part):
    shuffled = jax.random.permutation(jax.random.fold_in(key, 21), SLOTS).astype(jnp.int32)
    chosen = shuffled[:FRONTS]
    leading = chosen[0]
    partner = leading - leading % SLOT_DEV + (leading % SLOT_DEV + 1) % SLOT_DEV
    displaced = chosen[1]
    chosen = jnp.where(chosen == partner, displaced, chosen)
    chosen = chosen.at[1].set(partner)
    return chosen.astype(jnp.int32)


def set_ends(entries, rng, low, largest):
    extent = entries.shape
    place = [jax.random.randint(jax.random.fold_in(rng, axis), (), 0, extent[axis]) for axis in range(len(extent))]
    entries = entries.at[tuple(place)].set(low)
    longest = extent.index(max(extent))
    place[longest] = (place[longest] + 1) % extent[longest]
    return entries.at[tuple(place)].set(largest)


def steps_of(stream_key, extent, pieces, smallest, high):
    def one(dim, shards_of):
        steps = jax.random.uniform(jax.random.fold_in(jax.random.fold_in(stream_key, 6), dim), (shards_of,), jnp.float32, smallest / len(pieces), high / len(pieces))
        return jnp.repeat(jnp.exp(steps), extent[dim] // shards_of).reshape((-1,) + (1,) * (len(extent) - dim - 1))

    factor_of = one(*pieces[0])
    for cut in pieces[1:]:
        factor_of = factor_of * one(*cut)
    return factor_of


def centred(stream_key, shape, width, reach, pieces=(), kind=jnp.bfloat16):
    factor_of = steps_of(stream_key, shape, pieces, -0.22, 0.18) if pieces else 1.0
    array = jax.random.normal(stream_key, shape, jnp.float32) * width * factor_of
    return jnp.minimum(jnp.maximum(array, -reach), reach).astype(kind)


def setup_inputs(seed: int = 0) -> dict:
    seeds = jax.random.split(jax.random.key(seed), 7)
    return {
        "rhs": centred(seeds[0], (GROUPS, GCOLS, NROWS), 1.0, 6.0, ((0, 2), (1, 16)), jnp.float32),
        "pattern": set_ends((jax.random.randint(seeds[1], (RB, GROUPS), 0, 4) < 3).astype(jnp.int32), jax.random.fold_in(seeds[1], 1), 0, 1),
        "front_blocks": draw_front_blocks(jax.random.fold_in(seeds[6], 71), 0),
        "front_slot": draw_front_slot(jax.random.fold_in(seeds[6], 71), 0),
        "pivot_inverse": centred(seeds[4], (SLOTS, PIV, PIV), PIV ** -0.5, 0.375, ((0, 16),), jnp.float32),
        "update_factor": centred(seeds[5], (SLOTS, PIV, PIV), PIV ** -0.5, 0.375, ((0, 16),), jnp.float32),
    }


def reference(rhs, pattern, front_blocks, front_slot, pivot_inverse, update_factor):
    offsets = jnp.arange(BLOCK, dtype=jnp.int32)
    rows_of = (front_blocks[:, :, None] * BLOCK + offsets[None, None, :]).reshape(FRONTS, 4 * BLOCK).astype(jnp.int32)
    row_mask = jnp.repeat(pattern.astype(jnp.float32), BLOCK, axis=0)
    masked = rhs * jnp.transpose(row_mask)[:, None, :]
    strict_lower = jnp.tril(jnp.ones((PIV, PIV), jnp.float32), -1)
    identity = jnp.eye(PIV, dtype=jnp.float32)

    def one_front(result, front_index):
        rows = rows_of[front_index]
        slot_index = front_slot[front_index]
        pivots = jnp.take(masked, rows[:PIV], axis=2)
        inverse = identity + strict_lower * pivot_inverse[slot_index]
        solved = jnp.einsum("gcj,ij->gci", pivots, inverse, precision=lax.Precision.HIGHEST)
        update = jnp.einsum("gcj,ij->gci", solved, update_factor[slot_index], precision=lax.Precision.HIGHEST)
        result = result.at[:, :, rows[:PIV]].set(solved)
        result = result.at[:, :, rows[PIV:]].add(-update)
        return result, None

    result, _ = lax.scan(one_front, masked, jnp.arange(FRONTS, dtype=jnp.int32))
    return result
```

```python
import functools

import jax
import jax.numpy as jnp
from jax import lax
from jax.experimental import pallas as pl
from jax.experimental.pallas import tpu as pltpu
from jax.sharding import PartitionSpec as P

BLOCK = 128
COLS = 6
PAIR = 2
PARTS = 8
MESH = pl.DeviceIdType.MESH
WORK = ((0, 1), (2, 3), (6, 7), (4, 5))
GATHER = (0, 1, 2, 3, 6, 7, 4, 5)
OUT = (0, 1, 2, 3, 6, 7, 4, 5)
ROOT = (7, 6, 5, 4, 3, 2, 1, 0)


def split(value):
    high = value.astype(jnp.bfloat16)
    low = (value - high.astype(jnp.float32)).astype(jnp.bfloat16)
    return high, low


def times(x, high, low, inner):
    dims = (((1,), (inner,)), ((), ()))
    x_high, x_low = split(x)
    rows = x.shape[0]
    dot = functools.partial(lax.dot_general, dimension_numbers=dims, preferred_element_type=jnp.float32)
    both = dot(jnp.concatenate([x_high, x_low], axis=0), high)
    return both[:rows] + (both[rows:] + dot(x_high, low))


def kernel(
    n, fronts, blocks, chunk,
    rhs_hbm, pattern_hbm, fb_hbm, slot_hbm, row_hbm, inv_hbm, upd_hbm,
    out_ref,
    x, snd, rcv, back, pool, last, halves, inv, upd, wide, coef, fbv, slotv, table,
    pattern, fb, slot, front_of, src,
    local_sem, out_send, out_recv, back_send, back_recv, root_sem,
):
    me = lax.axis_index("rows")
    col = lax.axis_index("cols")
    slots = PAIR * n
    seps = blocks - 2 * fronts
    first = 6 * n
    few = n <= 16
    per = n // PARTS

    def offset(p):
        return PARTS * (p % per) + p // per

    def ahead(p):
        return lax.rem(me + offset(p), n)

    def behind(p):
        return lax.rem(me + n - offset(p), n)

    def place_of(away):
        return lax.rem(away, PARTS) * per + lax.div(away, PARTS)

    def device(index, core=col):
        return {"rows": index, "cols": core}

    lead, root = col == 1, jnp.logical_and(me == 0, col == 0)
    plain = jnp.logical_and(me != 0, col == 0)
    skipped = jnp.where(plain, place_of(me), -1)

    def span(begin, end, body):
        if few:
            for p in range(begin, end):
                body(p)
        else:
            def step(p, carry):
                body(p)
                return carry
            lax.fori_loop(begin, end, step, 0)

    def repeat(count, body, unroll=1):
        def step(i, carry):
            body(i)
            return carry
        lax.fori_loop(0, count, step, 0, unroll=unroll if few else 1)

    pieces = [
        (rhs_hbm, x), (pattern_hbm, pattern), (fb_hbm, fb), (slot_hbm, slot), (inv_hbm, inv), (upd_hbm, upd),
        (fb_hbm, fbv), (row_hbm, slotv),
    ]
    loads = [pltpu.make_async_copy(a, b, local_sem.at[i]) for i, (a, b) in enumerate(pieces)]
    for i in (3, 2, 1, 0):
        loads[i].start()

    barrier = pltpu.get_barrier_semaphore()

    def greet(p, core=col):
        pl.semaphore_signal(barrier, inc=1, device_id=device(ahead(p), core), device_id_type=MESH)

    span(1, n, lambda p: pl.when(jnp.logical_not(jnp.logical_and(col == 0, ahead(p) == 0)))(lambda: greet(p)))
    pl.when(lead)(lambda: pl.semaphore_signal(barrier, inc=1, device_id=device(0, 0), device_id_type=MESH))
    for i in (6, 7, 4, 5):
        loads[i].start()

    def total(count, term):
        if few:
            values = [term(i) for i in range(count)]
            while len(values) > 1:
                pairs = [a + b for a, b in zip(values[::2], values[1::2])]
                values = pairs + ([values[-1]] if len(values) % 2 else [])
            return values[0]
        return lax.fori_loop(0, count, lambda i, t: t + term(i), 0)

    loads[3].wait()

    def find_front(s):
        front_of[s] = jnp.minimum(total(fronts, lambda f: jnp.where(slot[f] == s, f, 0)), fronts - 1)

    repeat(slots, find_front, 2)
    for i in (2, 1, 0):
        loads[i].wait()

    def rows_of(b):
        return pl.ds(b, COLS, stride=blocks)

    def mask(b):
        x[rows_of(b), :] = x[rows_of(b), :] * pattern[b].astype(jnp.float32)

    repeat(blocks, mask, 16)

    def part(b, begin, count):
        return x[pl.ds(begin * blocks + b, count, stride=blocks), :]

    def pack(p):
        d = ahead(p)
        for k in range(PAIR):
            f = front_of[PAIR * d + k]
            b0, b1 = fb[0, f], fb[1, f]
            snd[p, k, 0] = part(b0, 0, 4)
            snd[p, k, 1, 0:2, :] = part(b0, 4, 2)
            snd[p, k, 1, 2:4, :] = part(b1, 0, 2)
            snd[p, k, 2] = part(b1, 2, 4)

    repeat(n, pack, 2)
    def fill(buffer, p):
        buffer[p] = snd[0]

    rcv[0] = snd[0]
    pl.when(col == 0)(lambda: fill(rcv, n))
    pl.when(plain)(lambda: fill(rcv, place_of(me)))

    def group(p):
        return p // per if isinstance(p, int) else lax.div(p, per)

    def send_out(p):
        pltpu.make_async_remote_copy(
            src_ref=snd.at[p], dst_ref=rcv.at[p], send_sem=out_send.at[group(p)], recv_sem=out_recv.at[group(p)],
            device_id=device(ahead(p)), device_id_type=MESH,
        ).start()

    def send_root(p):
        pltpu.make_async_remote_copy(
            src_ref=snd.at[p], dst_ref=rcv.at[n], send_sem=out_send.at[group(p)], recv_sem=root_sem.at[0],
            device_id=device(ahead(p), 1), device_id_type=MESH,
        ).start()

    pl.semaphore_wait(barrier, jnp.where(root, n, n - 1))

    @pl.when(jnp.logical_not(root))
    def _():
        for g in OUT:
            span(max(g * per, 1), (g + 1) * per, send_out)

    @pl.when(root)
    def _():
        for g in ROOT:
            span(g * per, (g + 1) * per, send_root)

    width = inv.shape[1]

    def widen():
        for i in (4, 5):
            loads[i].wait()
        row = lax.broadcasted_iota(jnp.int32, (width, width), 0)
        strict = row > lax.broadcasted_iota(jnp.int32, (width, width), 1)
        for k in range(PAIR):
            high, low = split(jnp.where(strict, inv[k], 0.0))
            wide[k, 0, :width], wide[k, 1, :width] = high, low
            wide[k, 0, width:], wide[k, 1, width:] = split(upd[k] + times(upd[k], high, low, 0))
        halves[...] = jnp.zeros(halves.shape, jnp.float32)

    tell = pltpu.make_async_copy(table, src, local_sem.at[8])

    def find_sources():
        for i in (6, 7):
            loads[i].wait()
        last[...] = jnp.zeros(last.shape, jnp.float32)
        pool[first:] = jnp.zeros((seps, 8, BLOCK), jnp.float32)

        owner = lax.div(slotv[...], PAIR)
        away = lax.rem(owner + n - me, n)
        position = lax.rem(away, PARTS) * per + lax.div(away, PARTS)
        place = 6 * position + 3 * lax.rem(slotv[...], PAIR)
        block = lax.broadcasted_iota(jnp.int32, (blocks, fronts), 0)
        value = jnp.zeros((blocks, fronts), jnp.int32)
        for h in range(2):
            named = fbv[h:h + 1, :]
            value = value + jnp.where(named == block, place + (h + 1), 0) + jnp.where(named < block, 4096, 0)
        value = jnp.sum(value.astype(jnp.float32), axis=1, keepdims=True).astype(jnp.int32)
        at, before = lax.rem(value, 4096), lax.div(value, 4096)
        own = lax.broadcasted_iota(jnp.int32, (blocks, 1), 0)
        found = jnp.where(at == 0, first + own - before, at - 1)
        lanes = table.shape[1]
        turned = jnp.where(
            lax.broadcasted_iota(jnp.int32, (blocks, lanes), 0) == lax.broadcasted_iota(jnp.int32, (blocks, lanes), 1),
            found, 0,
        )
        table[...] = jnp.sum(turned.astype(jnp.float32), axis=0, keepdims=True).astype(jnp.int32)
        tell.start()

    def landed(buffer, count, sem):
        view = buffer.at[pl.ds(0, count)]
        return pltpu.make_async_copy(view, view, sem)

    widen()
    find_sources()

    def remote(g):
        return per - 1 if isinstance(g, int) and g == 0 else per

    def source(b):
        return jnp.clip(src[0, b], 0, first + seps - 1)

    def weigh(c):
        rows = c * chunk + lax.broadcasted_iota(jnp.int32, (chunk, BLOCK), 0)

        def one_place(p):
            d = ahead(p)
            for k in range(PAIR):
                s = PAIR * d + k
                f = front_of[s]
                used = slot[f] == s
                for h in range(2):
                    named = jnp.where(used, source(fb[2 + h, f]) - first, -1)
                    coef[((c * n + p) * PAIR + k) * 2 + h] = jnp.where(rows == named, -1.0, 0.0)

        repeat(n, one_place, 4)

    def begin_with(b):
        keep = jnp.where(source(b) >= first, 1.0, 0.0)
        out_ref[rows_of(b), :] = x[rows_of(b), :] * keep

    def prepare():
        tell.wait()
        repeat(seps // chunk, weigh)
        repeat(blocks, begin_with, 16)

    def less(g, wait):
        none = jnp.logical_and(plain, lax.rem(me, PARTS) == g)
        if g > 0 or per > 2:
            pl.when(none)(lambda: wait(remote(g) - 1))
        pl.when(jnp.logical_not(none))(lambda: wait(remote(g)))

    def more(g, wait):
        if g > 0:
            wait(remote(g))
        else:
            pl.when(root)(lambda: wait(per))
            pl.when(jnp.logical_not(root))(lambda: wait(remote(g)))

    def work(i, names):
        parts = list(names)
        for g in parts:
            less(g, lambda count: landed(rcv, count, out_recv.at[g]).wait())
        count = len(parts) * per
        if parts[-1] == PARTS - 1:
            count += 1
            pl.when(lead)(lambda: landed(rcv, 1, root_sem.at[0]).wait())
        here = pl.ds(parts[0] * per, count)
        for k in range(PAIR):
            half = halves.at[PAIR * i + k]
            half[0, 0:count, 0:4, :] = rcv[here, k, 0]
            half[0, 0:count, 4:6, :] = rcv[here, k, 1, 0:2, :]
            half[1, 0:count, 0:2, :] = rcv[here, k, 1, 2:4, :]
            half[1, 0:count, 2:6, :] = rcv[here, k, 2]
            flat = [half[h, 0:count].reshape(8 * count, BLOCK) for h in range(2)]
            pivots = jnp.concatenate(flat, axis=1)
            both = times(pivots, wide[k, 0], wide[k, 1], 1)
            solved = pivots + both[:, :width]
            update = both[:, width:]
            quads = [
                part.reshape(count, 8, BLOCK)
                for part in (solved[:, :BLOCK], solved[:, BLOCK:], update[:, :BLOCK], update[:, BLOCK:])
            ]
            for t in range(3):
                back[here, 3 * k + t, 0:6, :] = quads[t][:, 0:6]
                back[here, 3 * k + t, 6:8, :] = quads[3][:, 2 * t:2 * t + 2]
        if parts[-1] == PARTS - 1:
            pl.when(lead)(send_to_root.start)
        for g in parts:
            send_back(g)

    def send_back(g):
        def one(p):
            pl.when(p != skipped)(lambda: pltpu.make_async_remote_copy(
                src_ref=back.at[p], dst_ref=pool.at[pl.ds(6 * p, 6)], send_sem=back_send.at[g], recv_sem=back_recv.at[g],
                device_id=device(behind(p)), device_id_type=MESH,
            ).start())

        span(max(g * per, 1), (g + 1) * per, one)
        if g == 0:
            pl.when(jnp.logical_not(root))(keep)

    send_to_root = pltpu.make_async_remote_copy(
        src_ref=back.at[n], dst_ref=pool.at[pl.ds(6 * place_of(me), 6)],
        send_sem=root_sem.at[1], recv_sem=back_recv.at[lax.rem(me, PARTS)],
        device_id=device(0, 0), device_id_type=MESH,
    )

    def keep():
        pool[0:6] = back[0]

    for i, names in enumerate(WORK):
        work(i, names)

    prepare()

    def gather(g):
        more(g, lambda count: landed(pool, 6 * count, back_recv.at[g]).wait())
        begin = PAIR * g * per
        for t in range(3):
            tiles = pool[pl.ds(3 * begin + t, PAIR * per, stride=3), 6:8, :]
            last[pl.ds(begin, PAIR * per), 2 * t:2 * t + 2, :] = tiles

        def add_up(c):
            def one_slot(o, accs):
                q = begin + o
                parts = (pool[3 * q + 2], last[q])
                for h in range(2):
                    row = (c * slots + q) * 2 + h
                    accs = tuple(a + coef[row, j:j + 1, :] * parts[h] for j, a in enumerate(accs))
                return accs

            at = first + c * chunk
            accs = tuple(pool[at + j] for j in range(chunk))
            accs = lax.fori_loop(0, PAIR * per, one_slot, accs, unroll=4 if few else 1)
            for j in range(chunk):
                pool[at + j] = accs[j]

        repeat(seps // chunk, add_up)

    for g in GATHER:
        gather(g)

    def put(b):
        out_ref[rows_of(b), :] = out_ref[rows_of(b), :] + pool[source(b), 0:6, :]

    repeat(blocks, put, 16)

    for g in range(PARTS):
        more(g, lambda count: landed(snd, count, out_send.at[g]).wait())
        less(g, lambda count: landed(back, count, back_send.at[g]).wait())
    pl.when(lead)(send_to_root.wait_send)


def on_device(n, rhs, pattern, front_blocks, front_slot, pivot_inverse, update_factor):
    fronts = front_blocks.shape[0]
    columns, total_rows = rhs.shape[1:]
    blocks = total_rows // BLOCK
    assert columns == COLS and pivot_inverse.shape[0] == PAIR and n & (n - 1) == 0 and n >= 16
    width = pivot_inverse.shape[1]
    slots = PAIR * n
    seps = blocks - 2 * fronts
    f32, i32 = jnp.float32, jnp.int32
    chunk = next(c for c in (16, 8, 4, 2, 1) if seps % c == 0)
    lanes = pl.cdiv(blocks, BLOCK) * BLOCK
    dma = pltpu.SemaphoreType.DMA
    result = pl.pallas_call(
        functools.partial(kernel, n, fronts, blocks, chunk),
        out_shape=pltpu.VMEM((columns * blocks, BLOCK), f32),
        in_specs=[pl.BlockSpec(memory_space=pl.ANY)] * 7,
        out_specs=pl.BlockSpec(memory_space=pltpu.VMEM),
        scratch_shapes=[
            pltpu.VMEM((columns * blocks, BLOCK), f32),
            pltpu.VMEM((n, PAIR, 3, 4, BLOCK), f32),
            pltpu.VMEM((n + 1, PAIR, 3, 4, BLOCK), f32),
            pltpu.VMEM((n + 1, 6, 8, BLOCK), f32),
            pltpu.VMEM((6 * n + seps, 8, BLOCK), f32),
            pltpu.VMEM((slots, 8, BLOCK), f32),
            pltpu.VMEM((PAIR * len(WORK), 2, 2 * n // PARTS + 1, 8, BLOCK), f32),
            pltpu.VMEM((PAIR, width, width), f32),
            pltpu.VMEM((PAIR, width, width), f32),
            pltpu.VMEM((PAIR, 2, 2 * width, width), jnp.bfloat16),
            pltpu.VMEM((seps // chunk * slots * 2, chunk, BLOCK), f32),
            pltpu.VMEM((4, fronts), i32),
            pltpu.VMEM((1, fronts), i32),
            pltpu.VMEM((1, lanes), i32),
            pltpu.SMEM((blocks,), i32),
            pltpu.SMEM((4, fronts), i32),
            pltpu.SMEM((fronts,), i32),
            pltpu.SMEM((slots,), i32),
            pltpu.SMEM((1, lanes), i32),
            dma((9,)),
            dma((PARTS,)),
            dma((PARTS,)),
            dma((PARTS,)),
            dma((PARTS,)),
            dma((2,)),
        ],
        compiler_params=pltpu.CompilerParams(collective_id=0, has_side_effects=True),
    )(
        rhs.reshape(columns * blocks, BLOCK),
        pattern.reshape(-1),
        front_blocks.T,
        front_slot,
        front_slot.reshape(1, -1),
        pivot_inverse,
        update_factor,
    )
    return result.reshape(1, columns, total_rows)


def solution(mesh):
    return jax.shard_map(
        functools.partial(on_device, mesh.shape["rows"]),
        mesh=mesh,
        in_specs=(
            P("cols", "rows", None),
            P(None, "cols"),
            P(),
            P(),
            P("rows", None, None),
            P("rows", None, None),
        ),
        out_specs=P("cols", "rows", None),
        check_vma=False,
    )
```

```python
import functools

import jax
import jax.numpy as jnp
from jax import lax
from jax.experimental import pallas as pl
from jax.experimental.pallas import tpu as pltpu
from jax.sharding import PartitionSpec as P

BLOCK = 128
COLS = 6
PAIR = 2
PARTS = 8
MESH = pl.DeviceIdType.MESH
WORK = ((0, 1), (2, 3), (6, 7), (4, 5))
GATHER = (0, 1, 2, 3, 6, 7, 4, 5)
OUT = (0, 1, 2, 3, 6, 7, 4, 5)
ROOT = (1, 0, 2, 3, 7, 6, 5, 4)


def split(value):
    high = value.astype(jnp.bfloat16)
    low = (value - high.astype(jnp.float32)).astype(jnp.bfloat16)
    return high, low


def times(x, high, low, inner):
    dims = (((1,), (inner,)), ((), ()))
    x_high, x_low = split(x)
    rows = x.shape[0]
    dot = functools.partial(lax.dot_general, dimension_numbers=dims, preferred_element_type=jnp.float32)
    both = dot(jnp.concatenate([x_high, x_low], axis=0), high)
    return both[:rows] + (both[rows:] + dot(x_high, low))


def kernel(
    n, fronts, blocks, chunk,
    rhs_hbm, pattern_hbm, fb_hbm, slot_hbm, row_hbm, inv_hbm, upd_hbm,
    out_ref,
    x, snd, rcv, back, pool, last, halves, inv, upd, wide, coef, fbv, slotv, table,
    pattern, fb, slot, front_of, src,
    local_sem, out_send, out_recv, back_send, back_recv, root_sem,
):
    me = lax.axis_index("rows")
    col = lax.axis_index("cols")
    slots = PAIR * n
    seps = blocks - 2 * fronts
    first = 6 * n
    few = n <= 16
    per = n // PARTS

    def offset(p):
        return PARTS * (p % per) + p // per

    def ahead(p):
        return lax.rem(me + offset(p), n)

    def behind(p):
        return lax.rem(me + n - offset(p), n)

    def place_of(away):
        return lax.rem(away, PARTS) * per + lax.div(away, PARTS)

    def device(index, core=col):
        return {"rows": index, "cols": core}

    lead, root = col == 1, jnp.logical_and(me == 0, col == 0)
    plain = jnp.logical_and(me != 0, col == 0)
    skipped = jnp.where(plain, place_of(me), -1)

    def span(begin, end, body):
        if few:
            for p in range(begin, end):
                body(p)
        else:
            def step(p, carry):
                body(p)
                return carry
            lax.fori_loop(begin, end, step, 0)

    def repeat(count, body, unroll=1):
        def step(i, carry):
            body(i)
            return carry
        lax.fori_loop(0, count, step, 0, unroll=unroll if few else 1)

    pieces = [
        (rhs_hbm, x), (pattern_hbm, pattern), (fb_hbm, fb), (slot_hbm, slot), (inv_hbm, inv), (upd_hbm, upd),
        (fb_hbm, fbv), (row_hbm, slotv),
    ]
    loads = [pltpu.make_async_copy(a, b, local_sem.at[i]) for i, (a, b) in enumerate(pieces)]
    loads[3].start()

    barrier = pltpu.get_barrier_semaphore()

    def greet(p, core=col):
        pl.semaphore_signal(barrier, inc=1, device_id=device(ahead(p), core), device_id_type=MESH)

    span(1, n, lambda p: pl.when(jnp.logical_not(jnp.logical_and(col == 0, ahead(p) == 0)))(lambda: greet(p)))
    pl.when(lead)(lambda: pl.semaphore_signal(barrier, inc=1, device_id=device(0, 0), device_id_type=MESH))
    for i in (0, 2, 1, 6, 7, 4, 5):
        loads[i].start()

    def total(count, term):
        if few:
            values = [term(i) for i in range(count)]
            while len(values) > 1:
                pairs = [a + b for a, b in zip(values[::2], values[1::2])]
                values = pairs + ([values[-1]] if len(values) % 2 else [])
            return values[0]
        return lax.fori_loop(0, count, lambda i, t: t + term(i), 0)

    loads[3].wait()

    def find_front(s):
        front_of[s] = jnp.minimum(total(fronts, lambda f: jnp.where(slot[f] == s, f, 0)), fronts - 1)

    repeat(slots, find_front, 2)
    for i in (2, 1, 0):
        loads[i].wait()

    def rows_of(b):
        return pl.ds(b, COLS, stride=blocks)

    def mask(b):
        x[rows_of(b), :] = x[rows_of(b), :] * pattern[b].astype(jnp.float32)

    repeat(blocks, mask, 16)

    def part(b, begin, count):
        return x[pl.ds(begin * blocks + b, count, stride=blocks), :]

    def pack(p):
        d = ahead(p)
        for k in range(PAIR):
            f = front_of[PAIR * d + k]
            b0, b1 = fb[0, f], fb[1, f]
            snd[p, k, 0] = part(b0, 0, 4)
            snd[p, k, 1, 0:2, :] = part(b0, 4, 2)
            snd[p, k, 1, 2:4, :] = part(b1, 0, 2)
            snd[p, k, 2] = part(b1, 2, 4)

    repeat(n, pack, 2)
    def fill(buffer, p):
        buffer[p] = snd[0]

    rcv[0] = snd[0]
    pl.when(col == 0)(lambda: fill(rcv, n))
    pl.when(plain)(lambda: fill(rcv, place_of(me)))

    def group(p):
        return p // per if isinstance(p, int) else lax.div(p, per)

    def send_out(p):
        pltpu.make_async_remote_copy(
            src_ref=snd.at[p], dst_ref=rcv.at[p], send_sem=out_send.at[0], recv_sem=out_recv.at[group(p)],
            device_id=device(ahead(p)), device_id_type=MESH,
        ).start()

    def send_root(p):
        pltpu.make_async_remote_copy(
            src_ref=snd.at[p], dst_ref=rcv.at[n], send_sem=out_send.at[0], recv_sem=root_sem.at[0],
            device_id=device(ahead(p), 1), device_id_type=MESH,
        ).start()

    pl.semaphore_wait(barrier, jnp.where(root, n, n - 1))

    @pl.when(jnp.logical_not(root))
    def _():
        for g in OUT:
            span(max(g * per, 1), (g + 1) * per, send_out)

    @pl.when(root)
    def _():
        for g in ROOT:
            span(g * per, (g + 1) * per, send_root)

    width = inv.shape[1]

    def widen():
        for i in (4, 5):
            loads[i].wait()
        row = lax.broadcasted_iota(jnp.int32, (width, width), 0)
        strict = row > lax.broadcasted_iota(jnp.int32, (width, width), 1)
        for k in range(PAIR):
            high, low = split(jnp.where(strict, inv[k], 0.0))
            wide[k, 0, :width], wide[k, 1, :width] = high, low
            wide[k, 0, width:], wide[k, 1, width:] = split(upd[k] + times(upd[k], high, low, 0))
        halves[...] = jnp.zeros(halves.shape, jnp.float32)

    tell = pltpu.make_async_copy(table, src, local_sem.at[8])

    def find_sources():
        for i in (6, 7):
            loads[i].wait()
        last[...] = jnp.zeros(last.shape, jnp.float32)
        pool[first:] = jnp.zeros((seps, 8, BLOCK), jnp.float32)

        owner = lax.div(slotv[...], PAIR)
        away = lax.rem(owner + n - me, n)
        position = lax.rem(away, PARTS) * per + lax.div(away, PARTS)
        place = 6 * position + 3 * lax.rem(slotv[...], PAIR)
        block = lax.broadcasted_iota(jnp.int32, (blocks, fronts), 0)
        value = jnp.zeros((blocks, fronts), jnp.int32)
        for h in range(2):
            named = fbv[h:h + 1, :]
            value = value + jnp.where(named == block, place + (h + 1), 0) + jnp.where(named < block, 4096, 0)
        value = jnp.sum(value.astype(jnp.float32), axis=1, keepdims=True).astype(jnp.int32)
        at, before = lax.rem(value, 4096), lax.div(value, 4096)
        own = lax.broadcasted_iota(jnp.int32, (blocks, 1), 0)
        found = jnp.where(at == 0, first + own - before, at - 1)
        lanes = table.shape[1]
        turned = jnp.where(
            lax.broadcasted_iota(jnp.int32, (blocks, lanes), 0) == lax.broadcasted_iota(jnp.int32, (blocks, lanes), 1),
            found, 0,
        )
        table[...] = jnp.sum(turned.astype(jnp.float32), axis=0, keepdims=True).astype(jnp.int32)
        tell.start()

    def landed(buffer, count, sem):
        view = buffer.at[pl.ds(0, count)]
        return pltpu.make_async_copy(view, view, sem)

    widen()
    find_sources()

    def remote(g):
        return per - 1 if isinstance(g, int) and g == 0 else per

    def source(b):
        return jnp.clip(src[0, b], 0, first + seps - 1)

    def weigh(c):
        rows = c * chunk + lax.broadcasted_iota(jnp.int32, (chunk, BLOCK), 0)

        def one_place(p):
            d = ahead(p)
            for k in range(PAIR):
                s = PAIR * d + k
                f = front_of[s]
                used = slot[f] == s
                for h in range(2):
                    named = jnp.where(used, source(fb[2 + h, f]) - first, -1)
                    coef[((c * n + p) * PAIR + k) * 2 + h] = jnp.where(rows == named, -1.0, 0.0)

        repeat(n, one_place, 4)

    def begin_with(b):
        keep = jnp.where(source(b) >= first, 1.0, 0.0)
        out_ref[rows_of(b), :] = x[rows_of(b), :] * keep

    def prepare():
        tell.wait()
        repeat(seps // chunk, weigh)
        repeat(blocks, begin_with, 16)

    def less(g, wait):
        none = jnp.logical_and(plain, lax.rem(me, PARTS) == g)
        if g > 0 or per > 2:
            pl.when(none)(lambda: wait(remote(g) - 1))
        pl.when(jnp.logical_not(none))(lambda: wait(remote(g)))

    def more(g, wait):
        if g > 0:
            wait(remote(g))
        else:
            pl.when(root)(lambda: wait(per))
            pl.when(jnp.logical_not(root))(lambda: wait(remote(g)))

    def work(i, names):
        parts = list(names)
        for g in parts:
            less(g, lambda count: landed(rcv, count, out_recv.at[g]).wait())
        count = len(parts) * per
        if parts[-1] == PARTS - 1:
            count += 1
            pl.when(lead)(lambda: landed(rcv, 1, root_sem.at[0]).wait())
        here = pl.ds(parts[0] * per, count)
        for k in range(PAIR):
            half = halves.at[PAIR * i + k]
            half[0, 0:count, 0:4, :] = rcv[here, k, 0]
            half[0, 0:count, 4:6, :] = rcv[here, k, 1, 0:2, :]
            half[1, 0:count, 0:2, :] = rcv[here, k, 1, 2:4, :]
            half[1, 0:count, 2:6, :] = rcv[here, k, 2]
            flat = [half[h, 0:count].reshape(8 * count, BLOCK) for h in range(2)]
            pivots = jnp.concatenate(flat, axis=1)
            both = times(pivots, wide[k, 0], wide[k, 1], 1)
            solved = pivots + both[:, :width]
            update = both[:, width:]
            quads = [
                part.reshape(count, 8, BLOCK)
                for part in (solved[:, :BLOCK], solved[:, BLOCK:], update[:, :BLOCK], update[:, BLOCK:])
            ]
            for t in range(3):
                back[here, 3 * k + t, 0:6, :] = quads[t][:, 0:6]
                back[here, 3 * k + t, 6:8, :] = quads[3][:, 2 * t:2 * t + 2]
        if parts[-1] == PARTS - 1:
            pl.when(lead)(send_to_root.start)
        for turn in range(2):
            for g in parts:
                send_back(g, turn)

    def send_back(g, turn):
        def one(p):
            pl.when(jnp.logical_and(p != skipped, (behind(p) < n // 4) == (turn == 0)))(lambda: pltpu.make_async_remote_copy(
                src_ref=back.at[p], dst_ref=pool.at[pl.ds(6 * p, 6)], send_sem=back_send.at[0], recv_sem=back_recv.at[g],
                device_id=device(behind(p)), device_id_type=MESH,
            ).start())

        span(max(g * per, 1), (g + 1) * per, one)
        if g == 0 and turn == 0:
            pl.when(jnp.logical_not(root))(keep)

    send_to_root = pltpu.make_async_remote_copy(
        src_ref=back.at[n], dst_ref=pool.at[pl.ds(6 * place_of(me), 6)],
        send_sem=root_sem.at[1], recv_sem=back_recv.at[lax.rem(me, PARTS)],
        device_id=device(0, 0), device_id_type=MESH,
    )

    def keep():
        pool[0:6] = back[0]

    for i, names in enumerate(WORK):
        work(i, names)

    prepare()

    def gather(g):
        more(g, lambda count: landed(pool, 6 * count, back_recv.at[g]).wait())
        begin = PAIR * g * per
        for t in range(3):
            tiles = pool[pl.ds(3 * begin + t, PAIR * per, stride=3), 6:8, :]
            last[pl.ds(begin, PAIR * per), 2 * t:2 * t + 2, :] = tiles

        def add_up(c):
            def one_slot(o, accs):
                q = begin + o
                parts = (pool[3 * q + 2], last[q])
                for h in range(2):
                    row = (c * slots + q) * 2 + h
                    accs = tuple(a + coef[row, j:j + 1, :] * parts[h] for j, a in enumerate(accs))
                return accs

            at = first + c * chunk
            accs = tuple(pool[at + j] for j in range(chunk))
            accs = lax.fori_loop(0, PAIR * per, one_slot, accs, unroll=4 if few else 1)
            for j in range(chunk):
                pool[at + j] = accs[j]

        repeat(seps // chunk, add_up)

    for g in GATHER:
        gather(g)

    def put(b):
        out_ref[rows_of(b), :] = out_ref[rows_of(b), :] + pool[source(b), 0:6, :]

    repeat(blocks, put, 16)

    pl.when(root)(lambda: landed(snd, n, out_send.at[0]).wait())
    pl.when(jnp.logical_not(root))(lambda: landed(snd, n - 1, out_send.at[0]).wait())
    pl.when(plain)(lambda: landed(back, n - 2, back_send.at[0]).wait())
    pl.when(jnp.logical_not(plain))(lambda: landed(back, n - 1, back_send.at[0]).wait())
    pl.when(lead)(send_to_root.wait_send)


def on_device(n, rhs, pattern, front_blocks, front_slot, pivot_inverse, update_factor):
    fronts = front_blocks.shape[0]
    columns, total_rows = rhs.shape[1:]
    blocks = total_rows // BLOCK
    assert columns == COLS and pivot_inverse.shape[0] == PAIR and n & (n - 1) == 0 and n >= 16
    width = pivot_inverse.shape[1]
    slots = PAIR * n
    seps = blocks - 2 * fronts
    f32, i32 = jnp.float32, jnp.int32
    chunk = next(c for c in (16, 8, 4, 2, 1) if seps % c == 0)
    lanes = pl.cdiv(blocks, BLOCK) * BLOCK
    dma = pltpu.SemaphoreType.DMA
    result = pl.pallas_call(
        functools.partial(kernel, n, fronts, blocks, chunk),
        out_shape=pltpu.VMEM((columns * blocks, BLOCK), f32),
        in_specs=[pl.BlockSpec(memory_space=pl.ANY)] * 7,
        out_specs=pl.BlockSpec(memory_space=pltpu.VMEM),
        scratch_shapes=[
            pltpu.VMEM((columns * blocks, BLOCK), f32),
            pltpu.VMEM((n, PAIR, 3, 4, BLOCK), f32),
            pltpu.VMEM((n + 1, PAIR, 3, 4, BLOCK), f32),
            pltpu.VMEM((n + 1, 6, 8, BLOCK), f32),
            pltpu.VMEM((6 * n + seps, 8, BLOCK), f32),
            pltpu.VMEM((slots, 8, BLOCK), f32),
            pltpu.VMEM((PAIR * len(WORK), 2, 2 * n // PARTS + 1, 8, BLOCK), f32),
            pltpu.VMEM((PAIR, width, width), f32),
            pltpu.VMEM((PAIR, width, width), f32),
            pltpu.VMEM((PAIR, 2, 2 * width, width), jnp.bfloat16),
            pltpu.VMEM((seps // chunk * slots * 2, chunk, BLOCK), f32),
            pltpu.VMEM((4, fronts), i32),
            pltpu.VMEM((1, fronts), i32),
            pltpu.VMEM((1, lanes), i32),
            pltpu.SMEM((blocks,), i32),
            pltpu.SMEM((4, fronts), i32),
            pltpu.SMEM((fronts,), i32),
            pltpu.SMEM((slots,), i32),
            pltpu.SMEM((1, lanes), i32),
            dma((9,)),
            dma((PARTS,)),
            dma((PARTS,)),
            dma((PARTS,)),
            dma((PARTS,)),
            dma((2,)),
        ],
        compiler_params=pltpu.CompilerParams(collective_id=0, has_side_effects=True),
    )(
        rhs.reshape(columns * blocks, BLOCK),
        pattern.reshape(-1),
        front_blocks.T,
        front_slot,
        front_slot.reshape(1, -1),
        pivot_inverse,
        update_factor,
    )
    return result.reshape(1, columns, total_rows)


def solution(mesh):
    return jax.shard_map(
        functools.partial(on_device, mesh.shape["rows"]),
        mesh=mesh,
        in_specs=(
            P("cols", "rows", None),
            P(None, "cols"),
            P(),
            P(),
            P("rows", None, None),
            P("rows", None, None),
        ),
        out_specs=P("cols", "rows", None),
        check_vma=False,
    )
```

```python
import functools

import jax
import jax.numpy as jnp
from jax import lax
from jax.experimental import pallas as pl
from jax.experimental.pallas import tpu as pltpu
from jax.sharding import PartitionSpec as P

BLOCK = 128
COLS = 6
PAIR = 2
PARTS = 8
MESH = pl.DeviceIdType.MESH
WORK = ((0, 1), (2, 3), (6, 7), (4, 5))
GATHER = (0, 1, 2, 3, 6, 7, 4, 5)
OUT = (1, 0, 2, 3, 6, 7, 4, 5)
ROOT = (1, 0, 2, 3, 7, 6, 5, 4)


def split(value):
    high = value.astype(jnp.bfloat16)
    low = (value - high.astype(jnp.float32)).astype(jnp.bfloat16)
    return high, low


def times(x, high, low, inner):
    dims = (((1,), (inner,)), ((), ()))
    x_high, x_low = split(x)
    rows = x.shape[0]
    dot = functools.partial(lax.dot_general, dimension_numbers=dims, preferred_element_type=jnp.float32)
    both = dot(jnp.concatenate([x_high, x_low], axis=0), high)
    return both[:rows] + (both[rows:] + dot(x_high, low))


def kernel(
    n, fronts, blocks, chunk,
    rhs_hbm, pattern_hbm, fb_hbm, slot_hbm, row_hbm, inv_hbm, upd_hbm,
    out_ref,
    x, snd, rcv, back, pool, last, halves, inv, upd, wide, coef, fbv, slotv, table,
    pattern, fb, slot, front_of, src,
    local_sem, out_send, out_recv, back_send, back_recv, root_sem,
):
    me = lax.axis_index("rows")
    col = lax.axis_index("cols")
    slots = PAIR * n
    seps = blocks - 2 * fronts
    first = 6 * n
    few = n <= 16
    per = n // PARTS

    def offset(p):
        return PARTS * (p % per) + p // per

    def ahead(p):
        return lax.rem(me + offset(p), n)

    def behind(p):
        return lax.rem(me + n - offset(p), n)

    def place_of(away):
        return lax.rem(away, PARTS) * per + lax.div(away, PARTS)

    def device(index, core=col):
        return {"rows": index, "cols": core}

    lead, root = col == 1, jnp.logical_and(me == 0, col == 0)
    plain = jnp.logical_and(me != 0, col == 0)
    skipped = jnp.where(plain, place_of(me), -1)

    def span(begin, end, body):
        if few:
            for p in range(begin, end):
                body(p)
        else:
            def step(p, carry):
                body(p)
                return carry
            lax.fori_loop(begin, end, step, 0)

    def repeat(count, body, unroll=1):
        def step(i, carry):
            body(i)
            return carry
        lax.fori_loop(0, count, step, 0, unroll=unroll if few else 1)

    pieces = [
        (rhs_hbm, x), (pattern_hbm, pattern), (fb_hbm, fb), (slot_hbm, slot), (inv_hbm, inv), (upd_hbm, upd),
        (fb_hbm, fbv), (row_hbm, slotv),
    ]
    loads = [pltpu.make_async_copy(a, b, local_sem.at[i]) for i, (a, b) in enumerate(pieces)]
    loads[3].start()

    barrier = pltpu.get_barrier_semaphore()

    def greet(p, core=col):
        pl.semaphore_signal(barrier, inc=1, device_id=device(ahead(p), core), device_id_type=MESH)

    span(1, n, lambda p: pl.when(jnp.logical_not(jnp.logical_and(col == 0, ahead(p) == 0)))(lambda: greet(p)))
    pl.when(lead)(lambda: pl.semaphore_signal(barrier, inc=1, device_id=device(0, 0), device_id_type=MESH))
    for i in (0, 2, 1, 6, 7, 4, 5):
        loads[i].start()

    def total(count, term):
        if few:
            values = [term(i) for i in range(count)]
            while len(values) > 1:
                pairs = [a + b for a, b in zip(values[::2], values[1::2])]
                values = pairs + ([values[-1]] if len(values) % 2 else [])
            return values[0]
        return lax.fori_loop(0, count, lambda i, t: t + term(i), 0)

    loads[3].wait()

    def find_front(s):
        front_of[s] = jnp.minimum(total(fronts, lambda f: jnp.where(slot[f] == s, f, 0)), fronts - 1)

    repeat(slots, find_front, 2)
    for i in (2, 1, 0):
        loads[i].wait()

    def rows_of(b):
        return pl.ds(b, COLS, stride=blocks)

    def mask(b):
        x[rows_of(b), :] = x[rows_of(b), :] * pattern[b].astype(jnp.float32)

    repeat(blocks, mask, 16)

    def part(b, begin, count):
        return x[pl.ds(begin * blocks + b, count, stride=blocks), :]

    def pack(p):
        d = ahead(p)
        for k in range(PAIR):
            f = front_of[PAIR * d + k]
            b0, b1 = fb[0, f], fb[1, f]
            snd[p, k, 0] = part(b0, 0, 4)
            snd[p, k, 1, 0:2, :] = part(b0, 4, 2)
            snd[p, k, 1, 2:4, :] = part(b1, 0, 2)
            snd[p, k, 2] = part(b1, 2, 4)

    repeat(n, pack, 2)
    def fill(buffer, p):
        buffer[p] = snd[0]

    rcv[0] = snd[0]
    pl.when(col == 0)(lambda: fill(rcv, n))
    pl.when(plain)(lambda: fill(rcv, place_of(me)))

    def group(p):
        return p // per if isinstance(p, int) else lax.div(p, per)

    def send_out(p):
        pltpu.make_async_remote_copy(
            src_ref=snd.at[p], dst_ref=rcv.at[p], send_sem=out_send.at[0], recv_sem=out_recv.at[group(p)],
            device_id=device(ahead(p)), device_id_type=MESH,
        ).start()

    def send_root(p):
        pltpu.make_async_remote_copy(
            src_ref=snd.at[p], dst_ref=rcv.at[n], send_sem=out_send.at[0], recv_sem=root_sem.at[0],
            device_id=device(ahead(p), 1), device_id_type=MESH,
        ).start()

    pl.semaphore_wait(barrier, jnp.where(root, n, n - 1))

    @pl.when(jnp.logical_not(root))
    def _():
        for g in OUT:
            span(max(g * per, 1), (g + 1) * per, send_out)

    @pl.when(root)
    def _():
        for g in ROOT:
            span(g * per, (g + 1) * per, send_root)

    width = inv.shape[1]

    def widen():
        for i in (4, 5):
            loads[i].wait()
        row = lax.broadcasted_iota(jnp.int32, (width, width), 0)
        strict = row > lax.broadcasted_iota(jnp.int32, (width, width), 1)
        for k in range(PAIR):
            high, low = split(jnp.where(strict, inv[k], 0.0))
            wide[k, 0, :width], wide[k, 1, :width] = high, low
            wide[k, 0, width:], wide[k, 1, width:] = split(upd[k] + times(upd[k], high, low, 0))
        halves[...] = jnp.zeros(halves.shape, jnp.float32)

    tell = pltpu.make_async_copy(table, src, local_sem.at[8])

    def find_sources():
        for i in (6, 7):
            loads[i].wait()
        last[...] = jnp.zeros(last.shape, jnp.float32)
        pool[first:] = jnp.zeros((seps, 8, BLOCK), jnp.float32)

        owner = lax.div(slotv[...], PAIR)
        away = lax.rem(owner + n - me, n)
        position = lax.rem(away, PARTS) * per + lax.div(away, PARTS)
        place = 6 * position + 3 * lax.rem(slotv[...], PAIR)
        block = lax.broadcasted_iota(jnp.int32, (blocks, fronts), 0)
        value = jnp.zeros((blocks, fronts), jnp.int32)
        for h in range(2):
            named = fbv[h:h + 1, :]
            value = value + jnp.where(named == block, place + (h + 1), 0) + jnp.where(named < block, 4096, 0)
        value = jnp.sum(value.astype(jnp.float32), axis=1, keepdims=True).astype(jnp.int32)
        at, before = lax.rem(value, 4096), lax.div(value, 4096)
        own = lax.broadcasted_iota(jnp.int32, (blocks, 1), 0)
        found = jnp.where(at == 0, first + own - before, at - 1)
        lanes = table.shape[1]
        turned = jnp.where(
            lax.broadcasted_iota(jnp.int32, (blocks, lanes), 0) == lax.broadcasted_iota(jnp.int32, (blocks, lanes), 1),
            found, 0,
        )
        table[...] = jnp.sum(turned.astype(jnp.float32), axis=0, keepdims=True).astype(jnp.int32)
        tell.start()

    def landed(buffer, count, sem):
        view = buffer.at[pl.ds(0, count)]
        return pltpu.make_async_copy(view, view, sem)

    widen()
    find_sources()

    def remote(g):
        return per - 1 if isinstance(g, int) and g == 0 else per

    def source(b):
        return jnp.clip(src[0, b], 0, first + seps - 1)

    def weigh(c):
        rows = c * chunk + lax.broadcasted_iota(jnp.int32, (chunk, BLOCK), 0)

        def one_place(p):
            d = ahead(p)
            for k in range(PAIR):
                s = PAIR * d + k
                f = front_of[s]
                used = slot[f] == s
                for h in range(2):
                    named = jnp.where(used, source(fb[2 + h, f]) - first, -1)
                    coef[((c * n + p) * PAIR + k) * 2 + h] = jnp.where(rows == named, -1.0, 0.0)

        repeat(n, one_place, 4)

    def begin_with(b):
        keep = jnp.where(source(b) >= first, 1.0, 0.0)
        out_ref[rows_of(b), :] = x[rows_of(b), :] * keep

    def prepare():
        tell.wait()
        repeat(seps // chunk, weigh)
        repeat(blocks, begin_with, 16)

    def less(g, wait):
        none = jnp.logical_and(plain, lax.rem(me, PARTS) == g)
        if g > 0 or per > 2:
            pl.when(none)(lambda: wait(remote(g) - 1))
        pl.when(jnp.logical_not(none))(lambda: wait(remote(g)))

    def more(g, wait):
        if g > 0:
            wait(remote(g))
        else:
            pl.when(root)(lambda: wait(per))
            pl.when(jnp.logical_not(root))(lambda: wait(remote(g)))

    def work(i, names):
        parts = list(names)
        for g in parts:
            less(g, lambda count: landed(rcv, count, out_recv.at[g]).wait())
        count = len(parts) * per
        if parts[-1] == PARTS - 1:
            count += 1
            pl.when(lead)(lambda: landed(rcv, 1, root_sem.at[0]).wait())
        here = pl.ds(parts[0] * per, count)
        for k in range(PAIR):
            half = halves.at[PAIR * i + k]
            half[0, 0:count, 0:4, :] = rcv[here, k, 0]
            half[0, 0:count, 4:6, :] = rcv[here, k, 1, 0:2, :]
            half[1, 0:count, 0:2, :] = rcv[here, k, 1, 2:4, :]
            half[1, 0:count, 2:6, :] = rcv[here, k, 2]
            flat = [half[h, 0:count].reshape(8 * count, BLOCK) for h in range(2)]
            pivots = jnp.concatenate(flat, axis=1)
            both = times(pivots, wide[k, 0], wide[k, 1], 1)
            solved = pivots + both[:, :width]
            update = both[:, width:]
            quads = [
                part.reshape(count, 8, BLOCK)
                for part in (solved[:, :BLOCK], solved[:, BLOCK:], update[:, :BLOCK], update[:, BLOCK:])
            ]
            for t in range(3):
                back[here, 3 * k + t, 0:6, :] = quads[t][:, 0:6]
                back[here, 3 * k + t, 6:8, :] = quads[3][:, 2 * t:2 * t + 2]
        if parts[-1] == PARTS - 1:
            pl.when(lead)(send_to_root.start)
        for turn in range(2):
            for g in parts:
                send_back(g, turn)

    def send_back(g, turn):
        def one(p):
            pl.when(jnp.logical_and(p != skipped, (behind(p) < n // 4) == (turn == 0)))(lambda: pltpu.make_async_remote_copy(
                src_ref=back.at[p], dst_ref=pool.at[pl.ds(6 * p, 6)], send_sem=back_send.at[0], recv_sem=back_recv.at[g],
                device_id=device(behind(p)), device_id_type=MESH,
            ).start())

        span(max(g * per, 1), (g + 1) * per, one)
        if g == 0 and turn == 0:
            pl.when(jnp.logical_not(root))(keep)

    send_to_root = pltpu.make_async_remote_copy(
        src_ref=back.at[n], dst_ref=pool.at[pl.ds(6 * place_of(me), 6)],
        send_sem=root_sem.at[1], recv_sem=back_recv.at[lax.rem(me, PARTS)],
        device_id=device(0, 0), device_id_type=MESH,
    )

    def keep():
        pool[0:6] = back[0]

    for i, names in enumerate(WORK):
        work(i, names)

    prepare()

    def gather(g):
        more(g, lambda count: landed(pool, 6 * count, back_recv.at[g]).wait())
        begin = PAIR * g * per
        for t in range(3):
            tiles = pool[pl.ds(3 * begin + t, PAIR * per, stride=3), 6:8, :]
            last[pl.ds(begin, PAIR * per), 2 * t:2 * t + 2, :] = tiles

        def add_up(c):
            def one_slot(o, accs):
                q = begin + o
                parts = (pool[3 * q + 2], last[q])
                for h in range(2):
                    row = (c * slots + q) * 2 + h
                    accs = tuple(a + coef[row, j:j + 1, :] * parts[h] for j, a in enumerate(accs))
                return accs

            at = first + c * chunk
            accs = tuple(pool[at + j] for j in range(chunk))
            accs = lax.fori_loop(0, PAIR * per, one_slot, accs, unroll=4 if few else 1)
            for j in range(chunk):
                pool[at + j] = accs[j]

        repeat(seps // chunk, add_up)

    for g in GATHER:
        gather(g)

    def put(b):
        out_ref[rows_of(b), :] = out_ref[rows_of(b), :] + pool[source(b), 0:6, :]

    repeat(blocks, put, 16)

    pl.when(root)(lambda: landed(snd, n, out_send.at[0]).wait())
    pl.when(jnp.logical_not(root))(lambda: landed(snd, n - 1, out_send.at[0]).wait())
    pl.when(plain)(lambda: landed(back, n - 2, back_send.at[0]).wait())
    pl.when(jnp.logical_not(plain))(lambda: landed(back, n - 1, back_send.at[0]).wait())
    pl.when(lead)(send_to_root.wait_send)


def on_device(n, rhs, pattern, front_blocks, front_slot, pivot_inverse, update_factor):
    fronts = front_blocks.shape[0]
    columns, total_rows = rhs.shape[1:]
    blocks = total_rows // BLOCK
    assert columns == COLS and pivot_inverse.shape[0] == PAIR and n & (n - 1) == 0 and n >= 16
    width = pivot_inverse.shape[1]
    slots = PAIR * n
    seps = blocks - 2 * fronts
    f32, i32 = jnp.float32, jnp.int32
    chunk = next(c for c in (16, 8, 4, 2, 1) if seps % c == 0)
    lanes = pl.cdiv(blocks, BLOCK) * BLOCK
    dma = pltpu.SemaphoreType.DMA
    result = pl.pallas_call(
        functools.partial(kernel, n, fronts, blocks, chunk),
        out_shape=pltpu.VMEM((columns * blocks, BLOCK), f32),
        in_specs=[pl.BlockSpec(memory_space=pl.ANY)] * 7,
        out_specs=pl.BlockSpec(memory_space=pltpu.VMEM),
        scratch_shapes=[
            pltpu.VMEM((columns * blocks, BLOCK), f32),
            pltpu.VMEM((n, PAIR, 3, 4, BLOCK), f32),
            pltpu.VMEM((n + 1, PAIR, 3, 4, BLOCK), f32),
            pltpu.VMEM((n + 1, 6, 8, BLOCK), f32),
            pltpu.VMEM((6 * n + seps, 8, BLOCK), f32),
            pltpu.VMEM((slots, 8, BLOCK), f32),
            pltpu.VMEM((PAIR * len(WORK), 2, 2 * n // PARTS + 1, 8, BLOCK), f32),
            pltpu.VMEM((PAIR, width, width), f32),
            pltpu.VMEM((PAIR, width, width), f32),
            pltpu.VMEM((PAIR, 2, 2 * width, width), jnp.bfloat16),
            pltpu.VMEM((seps // chunk * slots * 2, chunk, BLOCK), f32),
            pltpu.VMEM((4, fronts), i32),
            pltpu.VMEM((1, fronts), i32),
            pltpu.VMEM((1, lanes), i32),
            pltpu.SMEM((blocks,), i32),
            pltpu.SMEM((4, fronts), i32),
            pltpu.SMEM((fronts,), i32),
            pltpu.SMEM((slots,), i32),
            pltpu.SMEM((1, lanes), i32),
            dma((9,)),
            dma((PARTS,)),
            dma((PARTS,)),
            dma((PARTS,)),
            dma((PARTS,)),
            dma((2,)),
        ],
        compiler_params=pltpu.CompilerParams(collective_id=0, has_side_effects=True),
    )(
        rhs.reshape(columns * blocks, BLOCK),
        pattern.reshape(-1),
        front_blocks.T,
        front_slot,
        front_slot.reshape(1, -1),
        pivot_inverse,
        update_factor,
    )
    return result.reshape(1, columns, total_rows)


def solution(mesh):
    return jax.shard_map(
        functools.partial(on_device, mesh.shape["rows"]),
        mesh=mesh,
        in_specs=(
            P("cols", "rows", None),
            P(None, "cols"),
            P(),
            P(),
            P("rows", None, None),
            P("rows", None, None),
        ),
        out_specs=P("cols", "rows", None),
        check_vma=False,
    )
```
